256 devices in a mesh: section: 8 (over z_lo, x), dp: 32 (over z_hi, y, core).
Axes of the slice: x: 4, y: 4, z: 8 (z_hi: 4, z_lo: 2; z = z_hi * 2 + z_lo), core: 2. Of those that a mesh axis runs over, the one named last changes fastest.
Arguments:
- ln_input: bfloat16 [8, 4096, 12288], P('section', 'dp'), may hold values from -6 to 6
- ln_grad: bfloat16 [8, 4096, 12288], P('section', 'dp'), may hold values from -6 to 6
- top_grad: bfloat16 [8, 4096, 12288], P('section', 'dp'), may hold values from -6 to 6
- ln_gain: float32 [8, 12288], P('section'), may hold values from 0.1 to 1.9
- hidden: bfloat16 [8, 4096, 64], P('section', 'dp'), may hold values from -8 to 8
- master: float32 [8, 64, 12288], P('section', 'dp'), may hold values from -6 to 6
- moment: float32 [8, 64, 12288], P('section', 'dp'), may hold values from -6 to 6
- second: float32 [8, 64, 12288], P('section', 'dp'), may hold values from 0.1 to 4
Outputs:
- new_master: float32 [8, 64, 12288], P('section', 'dp')
- new_moment: float32 [8, 64, 12288], P('section', 'dp')
- new_second: float32 [8, 64, 12288], P('section', 'dp')
- weights: bfloat16 [8, 64, 12288], P('section')
The draws below stay inside these ranges and needn't reach their ends.
All inputs are finite; a program needn't handle non-finite values.
Results may differ from the reference program's by a relative error of at most 0.0078.
Values may be sent and summed in bfloat16 or wider, within the bound.
A program may use at most 64 MiB of HBM per device.

```python
import math
import jax
import jax.numpy as jnp
from jax import lax

D = 12288
STEP = 20
TOKENS = 4096
ROWS = 64
N_SECTION = 8


def draw_hidden(key, part):
    keys = jax.random.split(key, 4)
    base = jax.random.normal(keys[0], (N_SECTION, TOKENS, ROWS), jnp.float32)
    position = jnp.arange(ROWS, dtype=jnp.float32) / max(ROWS - 1, 1)
    level = jnp.arange(N_SECTION, dtype=jnp.float32) / max(N_SECTION - 1, 1)
    column = 3.0 ** position * jax.random.uniform(keys[3], (ROWS,), jnp.float32, 0.5, 1.5)
    scaled = base * column[None, None, :] * (3.0 ** level)[:, None, None] / math.sqrt(TOKENS)
    return jnp.clip(scaled, -8.0, 8.0).astype(jnp.bfloat16)


def levels(stream_key, extent, shards, least, top_value):
    factor_of = 1.0
    for dim, parts in shards:
        heights = jax.random.uniform(jax.random.fold_in(jax.random.fold_in(stream_key, 6), dim), (parts,), jnp.float32, least / len(shards), top_value / len(shards))
        factor_of = factor_of * jnp.repeat(jnp.exp(heights), extent[dim] // parts).reshape((-1,) + (1,) * (len(extent) - 1 - dim))
    return factor_of


def noise(stream_key, extent, deviation, bound, cuts=(), kind=jnp.bfloat16):
    level = levels(stream_key, extent, cuts, -0.22, 0.18) if cuts else 1.0
    array = jax.random.normal(stream_key, extent, jnp.float32) * deviation * level
    return jnp.minimum(jnp.maximum(array, -bound), bound).astype(kind)


def setup_inputs(seed: int = 0) -> dict:
    key_of = jax.random.split(jax.random.key(seed), 9)
    return {
        "ln_input": noise(key_of[0], (N_SECTION, TOKENS, D), 1.0, 6.0, ((0, 8), (1, 32))),
        "ln_grad": noise(key_of[1], (N_SECTION, TOKENS, D), 1.0, 6.0, ((0, 8), (1, 32))),
        "top_grad": noise(key_of[2], (N_SECTION, TOKENS, D), 1.0, 6.0, ((0, 8), (1, 32))),
        "ln_gain": jnp.clip(1.0 + 0.18 * jax.random.normal(key_of[3], (N_SECTION, D), jnp.float32), 0.1, 1.9),
        "hidden": draw_hidden(jax.random.fold_in(key_of[8], 71), 0),
        "master": noise(key_of[5], (N_SECTION, ROWS, D), 1.0, 6.0, ((0, 8), (1, 32)), jnp.float32),
        "moment": noise(key_of[6], (N_SECTION, ROWS, D), 1.0, 6.0, ((0, 8), (1, 32)), jnp.float32),
        "second": jnp.clip(jnp.exp(math.log(4.0) - 3.6888794 * jax.random.uniform(key_of[7], (N_SECTION, ROWS, D), jnp.float32) ** levels(key_of[7], (N_SECTION, ROWS, D), ((0, 8), (1, 32)), -0.2, 0.2)), 0.1, 4.0),
    }


def layer_back(ln_input, ln_grad, top_grad, ln_gain):
    values = ln_input.astype(jnp.float32)
    row_mean = lax.optimization_barrier(jnp.mean(values, axis=-1, keepdims=True))
    centred = values - row_mean
    inv_std = 1.0 / jnp.sqrt(lax.optimization_barrier(jnp.mean(centred * centred, axis=-1, keepdims=True)) + 1e-05)
    normed = centred * inv_std
    scaled = ln_grad.astype(jnp.float32) * ln_gain
    inner = scaled - lax.optimization_barrier(jnp.mean(scaled, axis=-1, keepdims=True)) - normed * lax.optimization_barrier(jnp.mean(scaled * normed, axis=-1, keepdims=True))
    return (top_grad.astype(jnp.float32) + inner * inv_std).astype(jnp.bfloat16)

def adam_update(grad, master, moment, second):
    new_moment = 0.9 * moment + 0.1 * grad
    new_second = 0.95 * second + 0.05 * grad * grad
    first_fix = 1.0 - 0.9 ** STEP
    second_fix = 1.0 - 0.95 ** STEP
    update = new_moment / first_fix / (jnp.sqrt(new_second / second_fix) + 1e-08)
    new_master = master - 0.05 * (update + 0.1 * master)
    return (new_master, new_moment, new_second)

def reference(ln_input, ln_grad, top_grad, ln_gain, hidden, master, moment, second):
    final_section = N_SECTION - 1

    def one_section(index):
        upper = jnp.minimum(index + 1, final_section)
        passed = layer_back(ln_input[upper], ln_grad[upper], top_grad[upper], ln_gain[upper])
        received = jnp.where(index == final_section, top_grad[index], passed)
        return lax.dot_general(hidden[index], received, (((0,), (0,)), ((), ())), preferred_element_type=jnp.float32)
    grad = lax.map(one_section, jnp.arange(N_SECTION, dtype=jnp.int32))
    new_master, new_moment, new_second = adam_update(grad, master, moment, second)
    weights = new_master.astype(jnp.bfloat16)
    return (new_master, new_moment, new_second, weights)
```

```python
import functools

import jax
import jax.numpy as jnp
from jax import lax
from jax.experimental import pallas as pl
from jax.experimental.pallas import tpu as pltpu
from jax.sharding import Mesh
from jax.sharding import PartitionSpec as P

STEP = 20
DP = ("zh", "y", "core")
MESH_ID = pl.DeviceIdType.MESH
F32, BF16 = jnp.float32, jnp.bfloat16
CHUNKS = 4
TILE = 512


def adam_update(grad, master, moment, second):
    new_moment = 0.9 * moment + 0.1 * grad
    new_second = 0.95 * second + 0.05 * grad * grad
    first_fix = 1.0 - 0.9**STEP
    second_fix = 1.0 - 0.95**STEP
    update = new_moment / first_fix / (jnp.sqrt(new_second / second_fix) + 1e-08)
    new_master = master - 0.05 * (update + 0.1 * master)
    return (new_master, new_moment, new_second)


def dot(a, b, dims=((1,), (0,)), precision=None):
    return lax.dot_general(a, b, (dims, ((), ())), preferred_element_type=F32, precision=precision)


def halves(v):
    high = v.astype(BF16)
    return high, (v - high.astype(F32)).astype(BF16)


def kernel(
    n_section,
    x_h, g_h, t_h, gain_h, hid_h, ms_h, mo_h, se_h,
    nms_o, nmo_o, nse_o, w_o,
    tx, gv, gain, hid_own, hid_in, ms, mo, se,
    lhs_tx, lhs_g, lhs_b, cst,
    p_own, p_snd, p_rcv, a_snd, a_rcv, b_snd, b_rcv, z_snd, z_rcv,
    nms, nmo, nse, agz, w8, wall, w_out,
    ld_sem, hid_s, hid_r, d_s, d_r, a_s, a_r, b_s, b_r, z_s, z_r, g_s, g_r, wy_s, wy_r, wd_s, wd_r, o_s,
):
    s = lax.axis_index("section")
    zh, y, core = lax.axis_index("zh"), lax.axis_index("y"), lax.axis_index("core")
    tokens, width = gv.shape
    n_chunk = z_rcv.shape[0]
    span = width // n_chunk
    has_below, has_above, is_last = s > 0, s < n_section - 1, s == n_section - 1
    y_pair, y_far, y_opp = y + 1 - 2 * lax.rem(y, 2), 3 - y, lax.rem(y + 2, 4)
    partner = (s, zh, y, 1 - core)

    def z_at(k):
        return lax.rem(zh + k, 4)

    def roles(c):
        return (y_pair, y_far) if c % 2 == 0 else (y_far, y_pair)

    def cols(c):
        return pl.ds(c * span, span)

    def load(which, c):
        if which == 0:
            return pltpu.make_async_copy(x_h.at[:, cols(c)], tx.at[pl.ds(tokens, tokens), cols(c)], ld_sem.at[0, c])
        if which == 1:
            return pltpu.make_async_copy(g_h.at[:, cols(c)], gv.at[:, cols(c)], ld_sem.at[1, c])
        return pltpu.make_async_copy(t_h.at[:, cols(c)], tx.at[pl.ds(0, tokens), cols(c)], ld_sem.at[2, c])

    small = [
        pltpu.make_async_copy(src, dst, ld_sem.at[3, i])
        for i, (src, dst) in enumerate([(ms_h, ms), (mo_h, mo), (se_h, se)])
    ]
    load_hid = pltpu.make_async_copy(hid_h, hid_own, ld_sem.at[3, 3])
    load_gain = pltpu.make_async_copy(gain_h, gain, ld_sem.at[4, 0])

    load_hid.start()

    @pl.when(is_last)
    def _():
        for c in range(n_chunk):
            load(2, c).start()

    @pl.when(has_below)
    def _():
        for c in range(n_chunk):
            load(0, c).start()
        load_gain.start()
        for c in range(n_chunk):
            load(1, c).start()

    @pl.when(jnp.logical_and(has_below, has_above))
    def _():
        for c in range(n_chunk):
            load(2, c).start()

    for copy in small:
        copy.start()

    barrier = pltpu.get_barrier_semaphore()

    def greet(device):
        pl.semaphore_signal(barrier, inc=1, device_id=device, device_id_type=MESH_ID)

    greet(partner)
    greet((s, zh, y_pair, core))
    greet((s, zh, y_far, core))
    for k in range(1, 4):
        greet((s, z_at(k), y, core))

    @pl.when(has_below)
    def _():
        for k in range(4):
            greet((s - 1, z_at(k), y, core))

    @pl.when(has_above)
    def _():
        for k in range(4):
            greet((s + 1, z_at(k), y, core))

    inner = jnp.logical_and(has_below, has_above)

    @pl.when(inner)
    def _():
        pl.semaphore_wait(barrier, 14)

    @pl.when(jnp.logical_not(inner))
    def _():
        pl.semaphore_wait(barrier, 10)

    def remote(src, dst, send, recv, device):
        return pltpu.make_async_remote_copy(
            src_ref=src, dst_ref=dst, send_sem=send, recv_sem=recv, device_id=device, device_id_type=MESH_ID
        )

    def send_hid():
        return remote(hid_own, hid_in, hid_s, hid_r, (s + 1, zh, y, core))

    load_hid.wait()

    @pl.when(has_above)
    def _():
        send_hid().start()

    def targets(rows):
        other = rows >> 5
        mine = core + other - 2 * core * other
        return ((rows >> 1) & 3) * 16 + ((rows >> 3) & 3) * 4 + mine * 2 + (rows & 1)

    rows = lax.broadcasted_iota(jnp.int32, (64, 64), 0)
    columns = lax.broadcasted_iota(jnp.int32, (64, 64), 1)
    gather_rows = jnp.where(targets(rows) == columns, 1.0, 0.0).astype(F32)
    spread_rows = jnp.where(targets(columns) == rows, 1.0, 0.0).astype(F32).astype(BF16)

    def turned(v):
        return dot(gather_rows.astype(BF16), v).astype(BF16)

    def keep_product(st, c, at, product):
        here = pl.ds(at, TILE)
        p_own[st, c, :, :, here] = product[:32].reshape(4, 8, TILE)
        p_snd[st, c, :, :, here] = product[32:].reshape(4, 8, TILE).astype(BF16)

    def d2d(st, c):
        return remote(p_snd.at[st, c], p_rcv.at[st, c], d_s.at[st, c], d_r.at[st, c], partner)

    def to_a(st, c):
        return remote(a_snd.at[st, c], a_rcv.at[st, c], a_s.at[st, c], a_r.at[st, c], (s, zh, roles(c)[0], core))

    def to_b(st, c):
        return remote(b_snd.at[st, c], b_rcv.at[st, c], b_s.at[st, c], b_r.at[st, c], (s, zh, roles(c)[1], core))

    def to_z(st, c, k):
        section = s - 1 if st == 0 else s
        return remote(
            z_snd.at[st, c, z_at(k)], z_rcv.at[c, zh], z_s.at[st, c, k], z_r.at[c, zh], (section, z_at(k), y, core)
        )

    def from_z(c, k):
        return remote(
            z_snd.at[0, c, z_at(k)], z_rcv.at[c, z_at(k)], z_s.at[0, c, k], z_r.at[c, z_at(k)], (s, z_at(1), y, core)
        )

    def gather_z(c, k):
        return remote(agz.at[c, zh], agz.at[c, zh], g_s.at[c, k - 1], g_r.at[c, zh], (s, z_at(k), y, core))

    def gathered_z(c, k):
        return remote(
            agz.at[c, zh], agz.at[c, z_at(k)], g_s.at[c, k - 1], g_r.at[c, z_at(k)], (s, z_at(k), y, core)
        )

    def along_y(c, which):
        a, b = roles(c)
        block, to = ((y, b), (y, a), (b, a))[which]
        return remote(
            wall.at[c, 0, block], wall.at[c, 0, block], wy_s.at[c, which], wy_r.at[c, which], (s, zh, to, core)
        )

    def arrived_y(c, which):
        a, b = roles(c)
        block = (b, a, y_opp)[which]
        return remote(
            wall.at[c, 0, block], wall.at[c, 0, block], wy_s.at[c, which], wy_r.at[c, which], (s, zh, b, core)
        )

    def over(c, which):
        a, b = roles(c)
        block = (y, b, a, y_opp)[which]
        return remote(
            wall.at[c, 0, block], wall.at[c, 1, block], wd_s.at[c, which], wd_r.at[c, which], partner
        )

    def last_product():
        lhs_b[...] = turned(hid_own[...])
        for c in range(n_chunk):
            load(2, c).wait()

            def step(j, _, c=c):
                at = pl.multiple_of(j * TILE, TILE)
                here = pl.ds(pl.multiple_of(c * span + j * TILE, TILE), TILE)
                keep_product(1, c, at, dot(lhs_b[...], tx[:tokens, here]))
                return 0

            lax.fori_loop(0, span // TILE, step, 0)
            d2d(1, c).start()

    def statistics():
        groups = span // 128
        half = tokens // 2
        sums = jnp.zeros((tokens, 128), F32)
        for c in range(n_chunk):
            load(0, c).wait()

            def step(j, acc, c=c):
                here = pl.ds(pl.multiple_of(c * span + j * 128, 128), 128)
                return acc + tx[tokens:, here].astype(F32)

            sums = lax.fori_loop(0, groups, step, sums)
        mean = jnp.sum(sums, axis=1, keepdims=True) * (1.0 / width)
        load_gain.wait()
        for c in range(n_chunk):
            load(1, c).wait()
        parts = []
        for h in range(2):
            low = h * half
            mean_b = jnp.broadcast_to(mean[low : low + half], (half, 128))
            zero = jnp.zeros((half, 128), F32)

            def step(j, acc, low=low, mean_b=mean_b):
                square, plain, cross = acc
                here = pl.ds(pl.multiple_of(j * 128, 128), 128)
                centred = tx[pl.ds(tokens + low, half), here].astype(F32) - mean_b
                scaled = gv[pl.ds(low, half), here].astype(F32) * gain[:, here]
                return (square + centred * centred, plain + scaled, cross + scaled * centred)

            acc = lax.fori_loop(0, width // 128, step, (zero, zero, zero))
            parts.append([jnp.sum(v, axis=1, keepdims=True) * (1.0 / width) for v in acc])
        var, mean_scaled, cross = (jnp.concatenate([p[i] for p in parts], axis=0) for i in range(3))
        inv = 1.0 / jnp.sqrt(var + 1e-05)
        lane = lax.broadcasted_iota(jnp.int32, (tokens, tokens), 1)
        table = jnp.zeros((tokens, tokens), F32)
        for i, column in enumerate((inv, inv * inv * inv * cross, mean_scaled, mean)):
            table = jnp.where(lane == i, column, table)
        table = table.T
        inv, along, mean_scaled, mean = (table[i : i + 1] for i in range(4))

        send = send_hid()
        send.wait_recv()
        hid = hid_in[...].astype(F32)
        g_high, g_low = halves(hid * inv)
        x_high, x_low = halves(hid * (-along))
        top = turned(hid_in[...])
        lhs_tx[:64, :tokens] = top
        lhs_tx[64:, :tokens] = jnp.zeros_like(top)
        lhs_tx[:64, tokens:] = turned(x_high)
        lhs_tx[64:, tokens:] = turned(x_low)
        lhs_g[:64] = turned(g_high)
        lhs_g[64:] = turned(g_low)
        g_sum = g_high.astype(F32) + g_low.astype(F32)
        x_sum = x_high.astype(F32) + x_low.astype(F32)
        shift = -(g_sum * mean_scaled + x_sum * mean)
        shifted = dot(gather_rows, shift, precision=lax.Precision.HIGHEST)
        cst[...] = jnp.broadcast_to(jnp.sum(shifted, axis=1, keepdims=True), cst.shape)

    def product(c):
        load_c = load(2, c)

        @pl.when(has_above)
        def _():
            load_c.wait()

        def step(j, _):
            at = pl.multiple_of(j * TILE, TILE)
            here = pl.ds(pl.multiple_of(c * span + j * TILE, TILE), TILE)
            plain = dot(lhs_tx[...], tx[:, here])
            scaled = dot(lhs_g[...], gv[:, here])
            whole = plain[:64] + plain[64:] + (scaled[:64] + scaled[64:]) * gain[:, here] + cst[:, :1]
            keep_product(0, c, at, whole)
            return 0

        lax.fori_loop(0, span // TILE, step, 0)
        d2d(0, c).start()

    def pair_sum(st, c):
        a, b = roles(c)
        d2d(st, c).wait_recv()
        for slot, block in enumerate((a, y_opp)):
            a_snd[st, c, slot] = (p_own[st, c, block] + p_rcv[st, c, block].astype(F32)).astype(BF16)
        to_a(st, c).start()

    def first_y(st, c):
        a, b = roles(c)
        to_a(st, c).wait_recv()
        b_snd[st, c] = (
            p_own[st, c, b] + p_rcv[st, c, b].astype(F32) + a_rcv[st, c, 1].astype(F32)
        ).astype(BF16)
        to_b(st, c).start()

    def second_y(st, c):
        to_b(st, c).wait_recv()
        total = (
            p_own[st, c, y] + p_rcv[st, c, y].astype(F32) + a_rcv[st, c, 0].astype(F32) + b_rcv[st, c].astype(F32)
        )
        for q in range(4):
            z_snd[st, c, q] = total[2 * q : 2 * q + 2].astype(BF16)
        if st == 1:
            z_rcv[c, zh] = z_snd[1, c, zh]
        for k in range(st, 4):
            to_z(st, c, k).start()

    def own_rows(c):
        for k in range(1, 4):
            from_z(c, k).wait_recv()

        @pl.when(has_above)
        def _():
            from_z(c, 0).wait_recv()

        grad = sum(z_rcv[c, q].astype(F32) for q in range(4))
        here = cols(c)
        new = adam_update(grad, ms[:, here], mo[:, here], se[:, here])
        nms[:, here], nmo[:, here], nse[:, here] = new
        agz[c, zh] = new[0].astype(BF16)
        for k in range(1, 4):
            gather_z(c, k).start()

    def weights_y(c):
        for k in range(1, 4):
            gathered_z(c, k).wait_recv()
        for q in range(4):
            w8[pl.ds(2 * q, 2), :] = agz[c, q].astype(F32)
        wall[c, 0, y] = w8[...].astype(BF16)
        along_y(c, 0).start()
        along_y(c, 1).start()
        over(c, 0).start()

    def weights_b(c):
        arrived_y(c, 0).wait_recv()
        along_y(c, 2).start()
        over(c, 1).start()

    def weights_a(c):
        arrived_y(c, 1).wait_recv()
        over(c, 2).start()
        arrived_y(c, 2).wait_recv()
        over(c, 3).start()

    def write_weights(c):
        for k in range(4):
            over(c, k).wait_recv()

        def step(j, _):
            at = pl.multiple_of(j * TILE, TILE)
            blocks = wall[c, :, :, :, pl.ds(at, TILE)].astype(F32).reshape(64, TILE).astype(BF16)
            here = pl.ds(pl.multiple_of(c * span + j * TILE, TILE), TILE)
            w_out[:, here] = dot(spread_rows, blocks).astype(BF16)
            return 0

        lax.fori_loop(0, span // TILE, step, 0)
        pltpu.make_async_copy(w_out.at[:, cols(c)], w_o.at[:, cols(c)], o_s.at[c]).start()

    for copy in small:
        copy.wait()

    pl.when(is_last)(last_product)
    pl.when(has_below)(statistics)

    gap = 6.4 / n_chunk
    below, last, always = has_below, is_last, None
    events = []
    for c in range(n_chunk):
        events += [
            (-1.0, c, last, functools.partial(pair_sum, 1, c)),
            (0.5 * gap * c, c, below, functools.partial(product, c)),
            (1.5 + 0.5 * gap * c, c, below, functools.partial(pair_sum, 0, c)),
            (0.8 + gap * c, c, last, functools.partial(first_y, 1, c)),
            (2.8 + gap * c, c, last, functools.partial(second_y, 1, c)),
            (5.0 + gap * c, c, below, functools.partial(first_y, 0, c)),
            (8.0 + gap * c, c, below, functools.partial(second_y, 0, c)),
            (12.5 + gap * c, c, always, functools.partial(own_rows, c)),
            (16.5 + gap * c, c, always, functools.partial(weights_y, c)),
            (19.0 + gap * c, c, always, functools.partial(weights_b, c)),
            (21.5 + gap * c, c, always, functools.partial(weights_a, c)),
            (23.0 + gap * c, c, always, functools.partial(write_weights, c)),
        ]
    for _, _, when, run in sorted(events, key=lambda e: e[:2]):
        if when is None:
            run()
        else:
            pl.when(when)(run)

    states = [
        pltpu.make_async_copy(src, dst, o_s.at[n_chunk + i])
        for i, (src, dst) in enumerate([(nms, nms_o), (nmo, nmo_o), (nse, nse_o)])
    ]
    for copy in states:
        copy.start()

    @pl.when(has_above)
    def _():
        send_hid().wait_send()

    def drain(st):
        for c in range(n_chunk):
            d2d(st, c).wait_send()
            to_a(st, c).wait_send()
            to_b(st, c).wait_send()
            for k in range(st, 4):
                to_z(st, c, k).wait_send()

    pl.when(has_below)(lambda: drain(0))
    pl.when(is_last)(lambda: drain(1))
    for c in range(n_chunk):
        for k in range(1, 4):
            gather_z(c, k).wait_send()
        for k in range(3):
            along_y(c, k).wait_send()
        for k in range(4):
            over(c, k).wait_send()
        pltpu.make_async_copy(w_out.at[:, cols(c)], w_o.at[:, cols(c)], o_s.at[c]).wait()
    for copy in states:
        copy.wait()


def shards(n_section, ln_input, ln_grad, top_grad, ln_gain, hidden, master, moment, second):
    tokens, width = ln_input.shape[1:]
    n_row = hidden.shape[2]
    own = master.shape[1]
    n, span = CHUNKS, width // CHUNKS
    dma = pltpu.SemaphoreType.DMA
    vmem = pltpu.VMEM
    any_space = pl.BlockSpec(memory_space=pl.ANY)
    state = jax.ShapeDtypeStruct((own, width), F32)
    outs = pl.pallas_call(
        functools.partial(kernel, n_section),
        out_shape=(state, state, state, jax.ShapeDtypeStruct((n_row, width), BF16)),
        in_specs=[any_space] * 8,
        out_specs=(any_space,) * 4,
        scratch_shapes=[
            vmem((2 * tokens, width), BF16),
            vmem((tokens, width), BF16),
            vmem((1, width), F32),
            vmem((n_row, tokens), BF16),
            vmem((n_row, tokens), BF16),
            vmem((own, width), F32),
            vmem((own, width), F32),
            vmem((own, width), F32),
            vmem((2 * n_row, 2 * tokens), BF16),
            vmem((2 * n_row, tokens), BF16),
            vmem((n_row, tokens), BF16),
            vmem((n_row, 128), F32),
            vmem((2, n, 4, 8, span), F32),
            vmem((2, n, 4, 8, span), BF16),
            vmem((2, n, 4, 8, span), BF16),
            vmem((2, n, 2, 8, span), BF16),
            vmem((2, n, 2, 8, span), BF16),
            vmem((2, n, 8, span), BF16),
            vmem((2, n, 8, span), BF16),
            vmem((2, n, 4, 2, span), BF16),
            vmem((n, 4, 2, span), BF16),
            vmem((own, width), F32),
            vmem((own, width), F32),
            vmem((own, width), F32),
            vmem((n, 4, 2, span), BF16),
            vmem((8, span), F32),
            vmem((n, 2, 4, 8, span), BF16),
            vmem((n_row, width), BF16),
            dma((5, max(n, 4))),
            dma(()),
            dma(()),
            dma((2, n)),
            dma((2, n)),
            dma((2, n)),
            dma((2, n)),
            dma((2, n)),
            dma((2, n)),
            dma((2, n, 4)),
            dma((n, 4)),
            dma((n, 3)),
            dma((n, 4)),
            dma((n, 3)),
            dma((n, 3)),
            dma((n, 4)),
            dma((n, 4)),
            dma((n + 3,)),
        ],
        compiler_params=pltpu.CompilerParams(
            collective_id=0, has_side_effects=True, vmem_limit_bytes=56 * 1024 * 1024
        ),
    )(ln_input[0], ln_grad[0], top_grad[0], ln_gain, hidden[0].T, master[0], moment[0], second[0])
    return tuple(out[None] for out in outs)


def solution(mesh):
    n_section = mesh.shape["section"]
    finer = Mesh(mesh.devices.reshape(n_section, 4, 4, 2), ("section", *DP))
    rows = P("section", DP, None)
    return jax.shard_map(
        functools.partial(shards, n_section),
        mesh=finer,
        in_specs=(rows, rows, rows, P("section", None), rows, rows, rows, rows),
        out_specs=(rows, rows, rows, P("section", None, None)),
        check_vma=False,
    )
```

```python
import functools

import jax
import jax.numpy as jnp
from jax import lax
from jax.experimental import pallas as pl
from jax.experimental.pallas import tpu as pltpu
from jax.sharding import Mesh
from jax.sharding import PartitionSpec as P

STEP = 20
DP = ("zh", "y", "core")
MESH_ID = pl.DeviceIdType.MESH
F32, BF16 = jnp.float32, jnp.bfloat16
CHUNKS = 4
TILE = 512


def adam_update(grad, master, moment, second):
    new_moment = 0.9 * moment + 0.1 * grad
    new_second = 0.95 * second + 0.05 * grad * grad
    first_fix = 1.0 - 0.9**STEP
    second_fix = 1.0 - 0.95**STEP
    update = new_moment / first_fix / (jnp.sqrt(new_second / second_fix) + 1e-08)
    new_master = master - 0.05 * (update + 0.1 * master)
    return (new_master, new_moment, new_second)


def dot(a, b, dims=((1,), (0,)), precision=None):
    return lax.dot_general(a, b, (dims, ((), ())), preferred_element_type=F32, precision=precision)


def halves(v):
    high = v.astype(BF16)
    return high, (v - high.astype(F32)).astype(BF16)


def kernel(
    n_section,
    x_h, g_h, t_h, gain_h, hid_h, ms_h, mo_h, se_h,
    nms, nmo, nse, w_out,
    tx, gv, gain, hid_own, hid_in, ms, mo, se,
    lhs_tx, lhs_g, lhs_b, cst,
    p_own, p_snd, p_rcv, a_snd, a_rcv, b_snd, b_rcv, z_snd, z_rcv,
    agz, w8, wall,
    ld_sem, hid_s, hid_r, d_s, d_r, a_s, a_r, b_s, b_r, z_s, z_r, g_s, g_r, wy_s, wy_r, wd_s, wd_r,
):
    s = lax.axis_index("section")
    zh, y, core = lax.axis_index("zh"), lax.axis_index("y"), lax.axis_index("core")
    tokens, width = gv.shape
    n_chunk = z_rcv.shape[0]
    span = width // n_chunk
    has_below, has_above, is_last = s > 0, s < n_section - 1, s == n_section - 1
    y_pair, y_far, y_opp = y + 1 - 2 * lax.rem(y, 2), 3 - y, lax.rem(y + 2, 4)
    partner = (s, zh, y, 1 - core)

    def z_at(k):
        return lax.rem(zh + k, 4)

    def roles(c):
        return (y_pair, y_far) if c % 2 == 0 else (y_far, y_pair)

    def cols(c):
        return pl.ds(c * span, span)

    def load(which, c):
        if which == 0:
            return pltpu.make_async_copy(x_h.at[:, cols(c)], tx.at[pl.ds(tokens, tokens), cols(c)], ld_sem.at[0, c])
        if which == 1:
            return pltpu.make_async_copy(g_h.at[:, cols(c)], gv.at[:, cols(c)], ld_sem.at[1, c])
        return pltpu.make_async_copy(t_h.at[:, cols(c)], tx.at[pl.ds(0, tokens), cols(c)], ld_sem.at[2, c])

    small = [
        pltpu.make_async_copy(src, dst, ld_sem.at[3, i])
        for i, (src, dst) in enumerate([(ms_h, ms), (mo_h, mo), (se_h, se)])
    ]
    load_hid = pltpu.make_async_copy(hid_h, hid_own, ld_sem.at[3, 3])
    load_gain = pltpu.make_async_copy(gain_h, gain, ld_sem.at[4, 0])

    load_hid.start()

    @pl.when(is_last)
    def _():
        for c in range(n_chunk):
            load(2, c).start()

    @pl.when(has_below)
    def _():
        for c in range(n_chunk):
            load(0, c).start()
        load_gain.start()
        for c in range(n_chunk):
            load(1, c).start()

    @pl.when(jnp.logical_and(has_below, has_above))
    def _():
        for c in range(n_chunk):
            load(2, c).start()

    for copy in small:
        copy.start()

    barrier = pltpu.get_barrier_semaphore()

    def greet(device):
        pl.semaphore_signal(barrier, inc=1, device_id=device, device_id_type=MESH_ID)

    greet(partner)
    greet((s, zh, y_pair, core))
    greet((s, zh, y_far, core))
    for k in range(1, 4):
        greet((s, z_at(k), y, core))

    @pl.when(has_below)
    def _():
        for k in range(4):
            greet((s - 1, z_at(k), y, core))

    @pl.when(has_above)
    def _():
        for k in range(4):
            greet((s + 1, z_at(k), y, core))

    def remote(src, dst, send, recv, device):
        return pltpu.make_async_remote_copy(
            src_ref=src, dst_ref=dst, send_sem=send, recv_sem=recv, device_id=device, device_id_type=MESH_ID
        )

    def send_hid():
        return remote(hid_own, hid_in, hid_s, hid_r, (s + 1, zh, y, core))

    def ready():
        inner = jnp.logical_and(has_below, has_above)

        @pl.when(has_above)
        def _():
            load_hid.wait()

        @pl.when(inner)
        def _():
            pl.semaphore_wait(barrier, 14)

        @pl.when(jnp.logical_not(inner))
        def _():
            pl.semaphore_wait(barrier, 10)

        @pl.when(has_above)
        def _():
            send_hid().start()

        @pl.when(is_last)
        def _():
            for c in range(n_chunk):
                d2d(1, c).start()

    def targets(rows):
        other = rows >> 5
        mine = core + other - 2 * core * other
        return ((rows >> 1) & 3) * 16 + ((rows >> 3) & 3) * 4 + mine * 2 + (rows & 1)

    rows = lax.broadcasted_iota(jnp.int32, (64, 64), 0)
    columns = lax.broadcasted_iota(jnp.int32, (64, 64), 1)
    gather_rows = jnp.where(targets(rows) == columns, 1.0, 0.0).astype(F32)
    spread_rows = jnp.where(targets(columns) == rows, 1.0, 0.0).astype(F32).astype(BF16)

    def turned(v):
        return dot(gather_rows.astype(BF16), v).astype(BF16)

    def keep_product(st, c, at, product):
        here = pl.ds(at, TILE)
        p_own[st, c, :, :, here] = product[:32].reshape(4, 8, TILE)
        p_snd[st, c, :, :, here] = product[32:].reshape(4, 8, TILE).astype(BF16)

    def d2d(st, c):
        return remote(p_snd.at[st, c], p_rcv.at[st, c], d_s.at[st, c], d_r.at[st, c], partner)

    def to_a(st, c):
        return remote(a_snd.at[st, c], a_rcv.at[st, c], a_s.at[st, c], a_r.at[st, c], (s, zh, roles(c)[0], core))

    def to_b(st, c):
        return remote(b_snd.at[st, c], b_rcv.at[st, c], b_s.at[st, c], b_r.at[st, c], (s, zh, roles(c)[1], core))

    def to_z(st, c, k):
        section = s - 1 if st == 0 else s
        return remote(
            z_snd.at[st, c, z_at(k)], z_rcv.at[c, zh], z_s.at[st, c, k], z_r.at[c, zh], (section, z_at(k), y, core)
        )

    def from_z(c, k):
        return remote(
            z_snd.at[0, c, z_at(k)], z_rcv.at[c, z_at(k)], z_s.at[0, c, k], z_r.at[c, z_at(k)], (s, z_at(1), y, core)
        )

    def gather_z(c, k):
        return remote(agz.at[c, zh], agz.at[c, zh], g_s.at[c, k - 1], g_r.at[c, zh], (s, z_at(k), y, core))

    def gathered_z(c, k):
        return remote(
            agz.at[c, zh], agz.at[c, z_at(k)], g_s.at[c, k - 1], g_r.at[c, z_at(k)], (s, z_at(k), y, core)
        )

    def along_y(c, which):
        a, b = roles(c)
        block, to = ((y, b), (y, a), (b, a))[which]
        return remote(
            wall.at[c, 0, block], wall.at[c, 0, block], wy_s.at[c, which], wy_r.at[c, which], (s, zh, to, core)
        )

    def arrived_y(c, which):
        a, b = roles(c)
        block = (b, a, y_opp)[which]
        return remote(
            wall.at[c, 0, block], wall.at[c, 0, block], wy_s.at[c, which], wy_r.at[c, which], (s, zh, b, core)
        )

    def over(c, which):
        a, b = roles(c)
        block = (y, b, a, y_opp)[which]
        return remote(
            wall.at[c, 0, block], wall.at[c, 1, block], wd_s.at[c, which], wd_r.at[c, which], partner
        )

    def last_product():
        load_hid.wait()
        lhs_b[...] = turned(hid_own[...])
        for c in range(n_chunk):
            load(2, c).wait()

            def step(j, _, c=c):
                at = pl.multiple_of(j * TILE, TILE)
                here = pl.ds(pl.multiple_of(c * span + j * TILE, TILE), TILE)
                keep_product(1, c, at, dot(lhs_b[...], tx[:tokens, here]))
                return 0

            lax.fori_loop(0, span // TILE, step, 0, unroll=2)

    def statistics():
        groups = span // 128
        sums = jnp.zeros((tokens, 128), F32)
        for c in range(n_chunk):
            load(0, c).wait()

            def step(j, acc, c=c):
                here = pl.ds(pl.multiple_of(c * span + j * 128, 128), 128)
                return acc + tx[tokens:, here].astype(F32)

            sums = lax.fori_loop(0, groups, step, sums, unroll=4)
        mean = jnp.sum(sums, axis=1, keepdims=True) * (1.0 / width)
        load_gain.wait()
        for c in range(n_chunk):
            load(1, c).wait()
        parts = []
        part = 32
        for low in range(0, tokens, part):
            mean_b = jnp.broadcast_to(mean[low : low + part], (part, 128))
            zero = jnp.zeros((part, 128), F32)

            def step(j, acc, low=low, mean_b=mean_b):
                square, plain, cross = acc
                here = pl.ds(pl.multiple_of(j * 128, 128), 128)
                centred = tx[pl.ds(tokens + low, part), here].astype(F32) - mean_b
                scaled = gv[pl.ds(low, part), here].astype(F32) * gain[:, here]
                return (square + centred * centred, plain + scaled, cross + scaled * centred)

            acc = lax.fori_loop(0, width // 128, step, (zero, zero, zero), unroll=8)
            parts.append([jnp.sum(v, axis=1, keepdims=True) * (1.0 / width) for v in acc])
            if low == 2 * part:
                with jax.named_scope("ready"):
                    ready()
        var, mean_scaled, cross = (jnp.concatenate([p[i] for p in parts], axis=0) for i in range(3))
        inv = 1.0 / jnp.sqrt(var + 1e-05)
        lane = lax.broadcasted_iota(jnp.int32, (tokens, tokens), 1)
        table = jnp.zeros((tokens, tokens), F32)
        for i, column in enumerate((inv, inv * inv * inv * cross, mean_scaled, mean)):
            table = jnp.where(lane == i, column, table)
        table = table.T
        inv, along, mean_scaled, mean = (table[i : i + 1] for i in range(4))

        with jax.named_scope("hid_wait"):
            send_hid().wait_recv()
        hid = hid_in[...].astype(F32)
        g_high, g_low = halves(hid * inv)
        x_high, x_low = halves(hid * (-along))
        top = turned(hid_in[...])
        lhs_tx[:64, :tokens] = top
        lhs_tx[64:, :tokens] = jnp.zeros_like(top)
        lhs_tx[:64, tokens:] = turned(x_high)
        lhs_tx[64:, tokens:] = turned(x_low)
        lhs_g[:64] = turned(g_high)
        lhs_g[64:] = turned(g_low)
        g_sum = g_high.astype(F32) + g_low.astype(F32)
        x_sum = x_high.astype(F32) + x_low.astype(F32)
        shift = -(g_sum * mean_scaled + x_sum * mean)
        shifted = dot(gather_rows, shift, precision=lax.Precision.HIGHEST)
        cst[...] = jnp.broadcast_to(jnp.sum(shifted, axis=1, keepdims=True), cst.shape)

    def product(c):
        load_c = load(2, c)

        @pl.when(has_above)
        def _():
            load_c.wait()

        def step(j, _):
            at = pl.multiple_of(j * TILE, TILE)
            here = pl.ds(pl.multiple_of(c * span + j * TILE, TILE), TILE)
            plain = dot(lhs_tx[...], tx[:, here])
            scaled = dot(lhs_g[...], gv[:, here])
            whole = plain[:64] + plain[64:] + (scaled[:64] + scaled[64:]) * gain[:, here] + cst[:, :1]
            keep_product(0, c, at, whole)
            return 0

        lax.fori_loop(0, span // TILE, step, 0, unroll=2)
        d2d(0, c).start()

    def pair_sum(st, c):
        a, b = roles(c)
        d2d(st, c).wait_recv()
        for slot, block in enumerate((a, y_opp)):
            a_snd[st, c, slot] = (p_own[st, c, block] + p_rcv[st, c, block].astype(F32)).astype(BF16)
        to_a(st, c).start()

    def first_y(st, c):
        a, b = roles(c)
        to_a(st, c).wait_recv()
        b_snd[st, c] = (
            p_own[st, c, b] + p_rcv[st, c, b].astype(F32) + a_rcv[st, c, 1].astype(F32)
        ).astype(BF16)
        to_b(st, c).start()

    def second_y(st, c):
        to_b(st, c).wait_recv()
        total = (
            p_own[st, c, y] + p_rcv[st, c, y].astype(F32) + a_rcv[st, c, 0].astype(F32) + b_rcv[st, c].astype(F32)
        )
        for q in range(4):
            z_snd[st, c, q] = total[2 * q : 2 * q + 2].astype(BF16)
        if st == 1:
            z_rcv[c, zh] = z_snd[1, c, zh]
        for k in range(st, 4):
            to_z(st, c, k).start()

    def own_rows(c):
        if c == 0:
            for copy in small:
                copy.wait()
        for k in range(1, 4):
            from_z(c, k).wait_recv()

        @pl.when(has_above)
        def _():
            from_z(c, 0).wait_recv()

        grad = sum(z_rcv[c, q].astype(F32) for q in range(4))
        here = cols(c)
        new = adam_update(grad, ms[:, here], mo[:, here], se[:, here])
        nms[:, here], nmo[:, here], nse[:, here] = new
        agz[c, zh] = new[0].astype(BF16)
        for k in range(1, 4):
            gather_z(c, k).start()

    def weights_y(c):
        for k in range(1, 4):
            gathered_z(c, k).wait_recv()
        for q in range(4):
            w8[pl.ds(2 * q, 2), :] = agz[c, q].astype(F32)
        wall[c, 0, y] = w8[...].astype(BF16)
        along_y(c, 0).start()
        along_y(c, 1).start()
        over(c, 0).start()

    def weights_b(c):
        arrived_y(c, 0).wait_recv()
        along_y(c, 2).start()
        over(c, 1).start()

    def weights_a(c):
        arrived_y(c, 1).wait_recv()
        over(c, 2).start()
        arrived_y(c, 2).wait_recv()
        over(c, 3).start()

    def write_weights(c):
        for k in range(4):
            over(c, k).wait_recv()

        def step(j, _):
            at = pl.multiple_of(j * TILE, TILE)
            blocks = wall[c, :, :, :, pl.ds(at, TILE)].astype(F32).reshape(64, TILE).astype(BF16)
            here = pl.ds(pl.multiple_of(c * span + j * TILE, TILE), TILE)
            w_out[:, here] = dot(spread_rows, blocks).astype(BF16)
            return 0

        lax.fori_loop(0, span // TILE, step, 0, unroll=2)

    with jax.named_scope("last_product"):
        pl.when(is_last)(last_product)
    with jax.named_scope("ready_0"):
        pl.when(jnp.logical_not(has_below))(ready)
    with jax.named_scope("statistics"):
        pl.when(has_below)(statistics)

    gap = 6.4 / n_chunk
    below, last, always = has_below, is_last, None
    events = []
    for c in range(n_chunk):
        events += [
            (-1.0, c, last, functools.partial(pair_sum, 1, c)),
            (0.5 * gap * c, c, below, functools.partial(product, c)),
            (1.5 + 0.5 * gap * c, c, below, functools.partial(pair_sum, 0, c)),
            (0.8 + gap * c, c, last, functools.partial(first_y, 1, c)),
            (2.8 + gap * c, c, last, functools.partial(second_y, 1, c)),
            (5.0 + gap * c, c, below, functools.partial(first_y, 0, c)),
            (8.0 + gap * c, c, below, functools.partial(second_y, 0, c)),
            (12.5 + gap * c, c, always, functools.partial(own_rows, c)),
            (16.5 + gap * c, c, always, functools.partial(weights_y, c)),
            (19.0 + gap * c, c, always, functools.partial(weights_b, c)),
            (21.5 + gap * c, c, always, functools.partial(weights_a, c)),
            (23.0 + gap * c, c, always, functools.partial(write_weights, c)),
        ]
    for _, c, when, run in sorted(events, key=lambda e: e[:2]):
        with jax.named_scope(f"{run.func.__name__}_{c}"):
            if when is None:
                run()
            else:
                pl.when(when)(run)

    @pl.when(has_above)
    def _():
        send_hid().wait_send()

    def drain(st):
        for c in range(n_chunk):
            d2d(st, c).wait_send()
            to_a(st, c).wait_send()
            to_b(st, c).wait_send()
            for k in range(st, 4):
                to_z(st, c, k).wait_send()

    pl.when(has_below)(lambda: drain(0))
    pl.when(is_last)(lambda: drain(1))
    for c in range(n_chunk):
        for k in range(1, 4):
            gather_z(c, k).wait_send()
        for k in range(3):
            along_y(c, k).wait_send()
        for k in range(4):
            over(c, k).wait_send()


def store(*refs):
    *refs, sems = refs
    copies = [pltpu.make_async_copy(refs[i], refs[4 + i], sems.at[i]) for i in range(4)]
    for copy in copies:
        copy.start()
    for copy in copies:
        copy.wait()


def shards(n_section, ln_input, ln_grad, top_grad, ln_gain, hidden, master, moment, second):
    tokens, width = ln_input.shape[1:]
    n_row = hidden.shape[2]
    own = master.shape[1]
    n, span = CHUNKS, width // CHUNKS
    dma = pltpu.SemaphoreType.DMA
    vmem = pltpu.VMEM
    any_space = pl.BlockSpec(memory_space=pl.ANY)
    results = (((own, width), F32),) * 3 + (((n_row, width), BF16),)
    outs = pl.pallas_call(
        functools.partial(kernel, n_section),
        out_shape=tuple(vmem(*r) for r in results),
        in_specs=[any_space] * 8,
        out_specs=(pl.BlockSpec(memory_space=vmem),) * 4,
        scratch_shapes=[
            vmem((2 * tokens, width), BF16),
            vmem((tokens, width), BF16),
            vmem((1, width), F32),
            vmem((n_row, tokens), BF16),
            vmem((n_row, tokens), BF16),
            vmem((own, width), F32),
            vmem((own, width), F32),
            vmem((own, width), F32),
            vmem((2 * n_row, 2 * tokens), BF16),
            vmem((2 * n_row, tokens), BF16),
            vmem((n_row, tokens), BF16),
            vmem((n_row, 128), F32),
            vmem((2, n, 4, 8, span), F32),
            vmem((2, n, 4, 8, span), BF16),
            vmem((2, n, 4, 8, span), BF16),
            vmem((2, n, 2, 8, span), BF16),
            vmem((2, n, 2, 8, span), BF16),
            vmem((2, n, 8, span), BF16),
            vmem((2, n, 8, span), BF16),
            vmem((2, n, 4, 2, span), BF16),
            vmem((n, 4, 2, span), BF16),
            vmem((n, 4, 2, span), BF16),
            vmem((8, span), F32),
            vmem((n, 2, 4, 8, span), BF16),
            dma((5, max(n, 4))),
            dma(()),
            dma(()),
            dma((2, n)),
            dma((2, n)),
            dma((2, n)),
            dma((2, n)),
            dma((2, n)),
            dma((2, n)),
            dma((2, n, 4)),
            dma((n, 4)),
            dma((n, 3)),
            dma((n, 4)),
            dma((n, 3)),
            dma((n, 3)),
            dma((n, 4)),
            dma((n, 4)),
        ],
        compiler_params=pltpu.CompilerParams(
            collective_id=0, has_side_effects=True, vmem_limit_bytes=56 * 1024 * 1024
        ),
    )(ln_input[0], ln_grad[0], top_grad[0], ln_gain, hidden[0].T, master[0], moment[0], second[0])
    outs = pl.pallas_call(
        store,
        out_shape=tuple(jax.ShapeDtypeStruct(*r) for r in results),
        in_specs=[pl.BlockSpec(memory_space=vmem)] * 4,
        out_specs=(any_space,) * 4,
        scratch_shapes=[dma((4,))],
    )(*(pltpu.with_memory_space_constraint(out, vmem) for out in outs))
    return tuple(out[None] for out in outs)


def solution(mesh):
    n_section = mesh.shape["section"]
    finer = Mesh(mesh.devices.reshape(n_section, 4, 4, 2), ("section", *DP))
    rows = P("section", DP, None)
    return jax.shard_map(
        functools.partial(shards, n_section),
        mesh=finer,
        in_specs=(rows, rows, rows, P("section", None), rows, rows, rows, rows),
        out_specs=(rows, rows, rows, P("section", None, None)),
        check_vma=False,
    )
```

```python
import functools

import jax
import jax.numpy as jnp
from jax import lax
from jax.experimental import pallas as pl
from jax.experimental.pallas import tpu as pltpu
from jax.sharding import Mesh
from jax.sharding import PartitionSpec as P

STEP = 20
DP = ("zh", "y", "core")
MESH_ID = pl.DeviceIdType.MESH
F32, BF16 = jnp.float32, jnp.bfloat16
CHUNKS = 8
TILE = 512


def adam_update(grad, master, moment, second):
    new_moment = 0.9 * moment + 0.1 * grad
    new_second = 0.95 * second + 0.05 * grad * grad
    first_fix = 1.0 - 0.9**STEP
    second_fix = 1.0 - 0.95**STEP
    update = new_moment / first_fix / (jnp.sqrt(new_second / second_fix) + 1e-08)
    new_master = master - 0.05 * (update + 0.1 * master)
    return (new_master, new_moment, new_second)


def dot(a, b, dims=((1,), (0,)), precision=None):
    return lax.dot_general(a, b, (dims, ((), ())), preferred_element_type=F32, precision=precision)


def halves(v):
    high = v.astype(BF16)
    return high, (v - high.astype(F32)).astype(BF16)


def kernel(
    n_section,
    x_h, g_h, t_h, gain_h, hid_h, ms_h, mo_h, se_h,
    nms, nmo, nse, w_out,
    tx, gv, gain, hid_own, hid_in, ms, mo, se,
    lhs_tx, lhs_g, lhs_b, cst,
    p_own, p_snd, p_rcv, a_snd, a_rcv, b_snd, b_rcv, z_snd, z_rcv,
    agz, w8, wall,
    ld_sem, hid_s, hid_r, d_s, d_r, a_s, a_r, b_s, b_r, z_s, z_r, g_s, g_r, wy_s, wy_r, wd_s, wd_r,
):
    s = lax.axis_index("section")
    zh, y, core = lax.axis_index("zh"), lax.axis_index("y"), lax.axis_index("core")
    tokens, width = gv.shape
    n_chunk = z_rcv.shape[0]
    span = width // n_chunk
    has_below, has_above, is_last = s > 0, s < n_section - 1, s == n_section - 1
    mine = (y, zh)
    pair_of, far_of, opp_of = ([f(i) for i in mine] for f in (lambda i: i + 1 - 2 * lax.rem(i, 2), lambda i: 3 - i, lambda i: lax.rem(i + 2, 4)))
    partner = (s, zh, y, 1 - core)

    def z_at(k):
        return lax.rem(zh + k, 4)

    def y_at(k):
        return lax.rem(y + k, 4)

    def roles(st, c):
        return (pair_of[st], far_of[st]) if c % 2 == 0 else (far_of[st], pair_of[st])

    def at(st, index):
        return (s, zh, index, core) if st == 0 else (s, index, y, core)

    def cols(c):
        return pl.ds(c * span, span)

    def load(which, c):
        if which == 0:
            return pltpu.make_async_copy(x_h.at[:, cols(c)], tx.at[pl.ds(tokens, tokens), cols(c)], ld_sem.at[0, c])
        if which == 1:
            return pltpu.make_async_copy(g_h.at[:, cols(c)], gv.at[:, cols(c)], ld_sem.at[1, c])
        return pltpu.make_async_copy(t_h.at[:, cols(c)], tx.at[pl.ds(0, tokens), cols(c)], ld_sem.at[2, c])

    small = [
        pltpu.make_async_copy(src, dst, ld_sem.at[3, i])
        for i, (src, dst) in enumerate([(ms_h, ms), (mo_h, mo), (se_h, se)])
    ]
    load_hid = pltpu.make_async_copy(hid_h, hid_own, ld_sem.at[3, 3])
    load_gain = pltpu.make_async_copy(gain_h, gain, ld_sem.at[4, 0])

    load_hid.start()

    @pl.when(is_last)
    def _():
        for c in range(n_chunk):
            load(2, c).start()

    @pl.when(has_below)
    def _():
        for c in range(n_chunk):
            load(0, c).start()
        load_gain.start()
        for c in range(n_chunk):
            load(1, c).start()

    @pl.when(jnp.logical_and(has_below, has_above))
    def _():
        for c in range(n_chunk):
            load(2, c).start()

    for copy in small:
        copy.start()

    barrier = pltpu.get_barrier_semaphore()

    def greet(device):
        pl.semaphore_signal(barrier, inc=1, device_id=device, device_id_type=MESH_ID)

    greet(partner)
    greet((s, zh, pair_of[0], core))
    greet((s, zh, far_of[0], core))
    for k in range(1, 4):
        greet((s, z_at(k), y, core))

    @pl.when(is_last)
    def _():
        greet((s, zh, opp_of[0], core))

    @pl.when(has_below)
    def _():
        for k in range(4):
            greet((s - 1, z_at(k), y, core))

    @pl.when(has_above)
    def _():
        for k in range(4):
            greet((s + 1, z_at(k), y, core))

    def remote(src, dst, send, recv, device):
        return pltpu.make_async_remote_copy(
            src_ref=src, dst_ref=dst, send_sem=send, recv_sem=recv, device_id=device, device_id_type=MESH_ID
        )

    def send_hid():
        return remote(hid_own, hid_in, hid_s, hid_r, (s + 1, zh, y, core))

    def ready():
        inner = jnp.logical_and(has_below, has_above)

        @pl.when(has_above)
        def _():
            load_hid.wait()

        @pl.when(inner)
        def _():
            pl.semaphore_wait(barrier, 14)

        @pl.when(jnp.logical_not(has_below))
        def _():
            pl.semaphore_wait(barrier, 10)

        @pl.when(is_last)
        def _():
            pl.semaphore_wait(barrier, 11)

        @pl.when(has_above)
        def _():
            send_hid().start()

        @pl.when(is_last)
        def _():
            for c in range(n_chunk):
                d2d(1, c).start()

    def targets(rows, y_shift=3, z_shift=1):
        other = rows >> 5
        whose = core + other - 2 * core * other
        return ((rows >> z_shift) & 3) * 16 + ((rows >> y_shift) & 3) * 4 + whose * 2 + (rows & 1)

    rows = lax.broadcasted_iota(jnp.int32, (64, 64), 0)
    columns = lax.broadcasted_iota(jnp.int32, (64, 64), 1)
    gather_rows = jnp.where(targets(rows) == columns, 1.0, 0.0).astype(F32)
    spread_rows = jnp.where(targets(columns) == rows, 1.0, 0.0).astype(F32).astype(BF16)

    def turned(v, order=gather_rows):
        return dot(order.astype(BF16), v).astype(BF16)

    def keep_product(st, c, at, product):
        here = pl.ds(at, TILE)
        p_own[st, c, :, :, here] = product[:32].reshape(4, 8, TILE)
        p_snd[st, c, :, :, here] = product[32:].reshape(4, 8, TILE).astype(BF16)

    def d2d(st, c):
        return remote(p_snd.at[st, c], p_rcv.at[st, c], d_s.at[st, c], d_r.at[st, c], partner)

    def to_a(st, c):
        return remote(a_snd.at[st, c], a_rcv.at[st, c], a_s.at[st, c], a_r.at[st, c], at(st, roles(st, c)[0]))

    def to_b(st, c):
        return remote(b_snd.at[st, c], b_rcv.at[st, c], b_s.at[st, c], b_r.at[st, c], at(st, roles(st, c)[1]))

    def to_owner(st, c, k):
        slot = z_at(k) if st == 0 else y_at(k)
        return remote(
            z_snd.at[st, c, slot],
            z_rcv.at[c, mine[1 - st]],
            z_s.at[st, c, k],
            z_r.at[c, mine[1 - st]],
            (s - 1, slot, y, core) if st == 0 else (s, zh, slot, core),
        )

    def to_own(st, c, k):
        slot = z_at(k) if st == 0 else y_at(k)
        return remote(z_snd.at[st, c, slot], z_rcv.at[c, slot], z_s.at[st, c, k], z_r.at[c, slot], partner)

    def gather_z(c, k):
        return remote(agz.at[c, zh], agz.at[c, zh], g_s.at[c, k - 1], g_r.at[c, zh], (s, z_at(k), y, core))

    def gathered_z(c, k):
        return remote(
            agz.at[c, zh], agz.at[c, z_at(k)], g_s.at[c, k - 1], g_r.at[c, z_at(k)], (s, z_at(k), y, core)
        )

    def along_y(c, which):
        a, b = roles(0, c)
        block, to = ((y, b), (y, a), (b, a))[which]
        return remote(
            wall.at[c, 0, block], wall.at[c, 0, block], wy_s.at[c, which], wy_r.at[c, which], (s, zh, to, core)
        )

    def arrived_y(c, which):
        a, b = roles(0, c)
        block = (b, a, opp_of[0])[which]
        return remote(
            wall.at[c, 0, block], wall.at[c, 0, block], wy_s.at[c, which], wy_r.at[c, which], (s, zh, b, core)
        )

    def over(c, which):
        a, b = roles(0, c)
        block = (y, b, a, opp_of[0])[which]
        return remote(
            wall.at[c, 0, block], wall.at[c, 1, block], wd_s.at[c, which], wd_r.at[c, which], partner
        )

    def last_product():
        load_hid.wait()
        lhs_b[...] = turned(hid_own[...], jnp.where(targets(rows, 1, 3) == columns, 1.0, 0.0))
        for c in range(n_chunk):
            load(2, c).wait()

            def step(j, _, c=c):
                at = pl.multiple_of(j * TILE, TILE)
                here = pl.ds(pl.multiple_of(c * span + j * TILE, TILE), TILE)
                keep_product(1, c, at, dot(lhs_b[...], tx[:tokens, here]))
                return 0

            lax.fori_loop(0, span // TILE, step, 0, unroll=2)

    def statistics():
        groups = span // 128
        sums = jnp.zeros((tokens, 128), F32)
        for c in range(n_chunk):
            load(0, c).wait()

            def step(j, acc, c=c):
                here = pl.ds(pl.multiple_of(c * span + j * 128, 128), 128)
                return acc + tx[tokens:, here].astype(F32)

            sums = lax.fori_loop(0, groups, step, sums, unroll=4)
        mean = jnp.sum(sums, axis=1, keepdims=True) * (1.0 / width)
        load_gain.wait()
        for c in range(n_chunk):
            load(1, c).wait()
        parts = []
        part = 32
        for low in range(0, tokens, part):
            mean_b = jnp.broadcast_to(mean[low : low + part], (part, 128))
            zero = jnp.zeros((part, 128), F32)

            def step(j, acc, low=low, mean_b=mean_b):
                square, plain, cross = acc
                here = pl.ds(pl.multiple_of(j * 128, 128), 128)
                centred = tx[pl.ds(tokens + low, part), here].astype(F32) - mean_b
                scaled = gv[pl.ds(low, part), here].astype(F32) * gain[:, here]
                return (square + centred * centred, plain + scaled, cross + scaled * centred)

            acc = lax.fori_loop(0, width // 128, step, (zero, zero, zero), unroll=8)
            parts.append([jnp.sum(v, axis=1, keepdims=True) * (1.0 / width) for v in acc])
            if low == 2 * part:
                with jax.named_scope("ready"):
                    ready()
        var, mean_scaled, cross = (jnp.concatenate([p[i] for p in parts], axis=0) for i in range(3))
        inv = 1.0 / jnp.sqrt(var + 1e-05)
        lane = lax.broadcasted_iota(jnp.int32, (tokens, tokens), 1)
        table = jnp.zeros((tokens, tokens), F32)
        for i, column in enumerate((inv, inv * inv * inv * cross, mean_scaled, mean)):
            table = jnp.where(lane == i, column, table)
        table = table.T
        inv, along, mean_scaled, mean = (table[i : i + 1] for i in range(4))

        with jax.named_scope("pair_b"):

            @pl.when(is_last)
            def _():
                for c in range(n_chunk):
                    pair_sum(1, c)

        with jax.named_scope("hid_wait"):
            send_hid().wait_recv()
        hid = hid_in[...].astype(F32)
        g_high, g_low = halves(hid * inv)
        x_high, x_low = halves(hid * (-along))
        top = turned(hid_in[...])
        lhs_tx[:64, :tokens] = top
        lhs_tx[64:, :tokens] = jnp.zeros_like(top)
        lhs_tx[:64, tokens:] = turned(x_high)
        lhs_tx[64:, tokens:] = turned(x_low)
        lhs_g[:64] = turned(g_high)
        lhs_g[64:] = turned(g_low)
        g_sum = g_high.astype(F32) + g_low.astype(F32)
        x_sum = x_high.astype(F32) + x_low.astype(F32)
        shift = -(g_sum * mean_scaled + x_sum * mean)
        shifted = dot(gather_rows, shift, precision=lax.Precision.HIGHEST)
        cst[...] = jnp.broadcast_to(jnp.sum(shifted, axis=1, keepdims=True), cst.shape)

    def product(c):
        load_c = load(2, c)

        @pl.when(has_above)
        def _():
            load_c.wait()

        def step(j, _):
            at = pl.multiple_of(j * TILE, TILE)
            here = pl.ds(pl.multiple_of(c * span + j * TILE, TILE), TILE)
            plain = dot(lhs_tx[...], tx[:, here])
            scaled = dot(lhs_g[...], gv[:, here])
            whole = plain[:64] + plain[64:] + (scaled[:64] + scaled[64:]) * gain[:, here] + cst[:, :1]
            keep_product(0, c, at, whole)
            return 0

        lax.fori_loop(0, span // TILE, step, 0, unroll=2)
        d2d(0, c).start()

    def pair_sum(st, c):
        a = roles(st, c)[0]
        d2d(st, c).wait_recv()
        for slot, block in enumerate((a, opp_of[st])):
            a_snd[st, c, slot] = (p_own[st, c, block] + p_rcv[st, c, block].astype(F32)).astype(BF16)
        to_a(st, c).start()

    def first_y(st, c):
        b = roles(st, c)[1]
        to_a(st, c).wait_recv()
        b_snd[st, c] = (
            p_own[st, c, b] + p_rcv[st, c, b].astype(F32) + a_rcv[st, c, 1].astype(F32)
        ).astype(BF16)
        to_b(st, c).start()

    def second_y(st, c):
        to_b(st, c).wait_recv()
        total = (
            p_own[st, c, mine[st]]
            + p_rcv[st, c, mine[st]].astype(F32)
            + a_rcv[st, c, 0].astype(F32)
            + b_rcv[st, c].astype(F32)
        )
        for q in range(4):
            z_snd[st, c, q] = total[2 * q : 2 * q + 2].astype(BF16)
        if st == 1:
            z_rcv[c, y] = z_snd[1, c, y]
        for k in range(st, 4):
            to_owner(st, c, k).start()

    def own_rows(c):
        if c == 0:
            for copy in small:
                copy.wait()

        @pl.when(has_above)
        def _():
            for k in range(4):
                to_own(0, c, k).wait_recv()

        @pl.when(is_last)
        def _():
            for k in range(1, 4):
                to_own(1, c, k).wait_recv()

        grad = sum(z_rcv[c, q].astype(F32) for q in range(4))
        here = cols(c)
        new = adam_update(grad, ms[:, here], mo[:, here], se[:, here])
        nms[:, here], nmo[:, here], nse[:, here] = new
        agz[c, zh] = new[0].astype(BF16)
        for k in range(1, 4):
            gather_z(c, k).start()

    def weights_y(c):
        for k in range(1, 4):
            gathered_z(c, k).wait_recv()
        for q in range(4):
            w8[pl.ds(2 * q, 2), :] = agz[c, q].astype(F32)
        wall[c, 0, y] = w8[...].astype(BF16)
        along_y(c, 0).start()
        along_y(c, 1).start()
        over(c, 0).start()

    def weights_b(c):
        arrived_y(c, 0).wait_recv()
        along_y(c, 2).start()
        over(c, 1).start()

    def weights_a(c):
        arrived_y(c, 1).wait_recv()
        over(c, 2).start()
        arrived_y(c, 2).wait_recv()
        over(c, 3).start()

    def write_weights(c):
        for k in range(4):
            over(c, k).wait_recv()

        def step(j, _):
            at = pl.multiple_of(j * TILE, TILE)
            blocks = wall[c, :, :, :, pl.ds(at, TILE)].astype(F32).reshape(64, TILE).astype(BF16)
            here = pl.ds(pl.multiple_of(c * span + j * TILE, TILE), TILE)
            w_out[:, here] = dot(spread_rows, blocks).astype(BF16)
            return 0

        lax.fori_loop(0, span // TILE, step, 0, unroll=2)

    with jax.named_scope("last_product"):
        pl.when(is_last)(last_product)
    with jax.named_scope("ready_0"):
        pl.when(jnp.logical_not(has_below))(ready)
    with jax.named_scope("statistics"):
        pl.when(has_below)(statistics)

    below, last, always = has_below, is_last, None
    events = []
    for c in range(n_chunk):
        part = c / n_chunk
        events += [
            (0 + part, c, below, functools.partial(product, c)),
            (0.4 + part, c, below, functools.partial(pair_sum, 0, c)),
            (2 + part, c, last, functools.partial(first_y, 1, c)),
            (3 + part, c, below, functools.partial(first_y, 0, c)),
            (4 + part, c, last, functools.partial(second_y, 1, c)),
            (5 + part, c, below, functools.partial(second_y, 0, c)),
            (6 + part, c, always, functools.partial(own_rows, c)),
            (7 + part, c, always, functools.partial(weights_y, c)),
            (8 + part, c, always, functools.partial(weights_b, c)),
            (9 + part, c, always, functools.partial(weights_a, c)),
            (9.4 + part, c, always, functools.partial(write_weights, c)),
        ]
    for _, c, when, run in sorted(events, key=lambda e: e[:2]):
        with jax.named_scope(f"{run.func.__name__}_{c}"):
            if when is None:
                run()
            else:
                pl.when(when)(run)

    @pl.when(has_above)
    def _():
        send_hid().wait_send()

    def drain(st):
        for c in range(n_chunk):
            d2d(st, c).wait_send()
            to_a(st, c).wait_send()
            to_b(st, c).wait_send()
            for k in range(st, 4):
                to_owner(st, c, k).wait_send()

    pl.when(has_below)(lambda: drain(0))
    pl.when(is_last)(lambda: drain(1))
    for c in range(n_chunk):
        for k in range(1, 4):
            gather_z(c, k).wait_send()
        for k in range(3):
            along_y(c, k).wait_send()
        for k in range(4):
            over(c, k).wait_send()


def store(*refs):
    *refs, sems = refs
    copies = [pltpu.make_async_copy(refs[i], refs[4 + i], sems.at[i]) for i in range(4)]
    for copy in copies:
        copy.start()
    for copy in copies:
        copy.wait()


def shards(n_section, ln_input, ln_grad, top_grad, ln_gain, hidden, master, moment, second):
    tokens, width = ln_input.shape[1:]
    n_row = hidden.shape[2]
    own = master.shape[1]
    n, span = CHUNKS, width // CHUNKS
    dma = pltpu.SemaphoreType.DMA
    vmem = pltpu.VMEM
    any_space = pl.BlockSpec(memory_space=pl.ANY)
    results = (((own, width), F32),) * 3 + (((n_row, width), BF16),)
    outs = pl.pallas_call(
        functools.partial(kernel, n_section),
        out_shape=tuple(vmem(*r) for r in results),
        in_specs=[any_space] * 8,
        out_specs=(pl.BlockSpec(memory_space=vmem),) * 4,
        scratch_shapes=[
            vmem((2 * tokens, width), BF16),
            vmem((tokens, width), BF16),
            vmem((1, width), F32),
            vmem((n_row, tokens), BF16),
            vmem((n_row, tokens), BF16),
            vmem((own, width), F32),
            vmem((own, width), F32),
            vmem((own, width), F32),
            vmem((2 * n_row, 2 * tokens), BF16),
            vmem((2 * n_row, tokens), BF16),
            vmem((n_row, tokens), BF16),
            vmem((n_row, 128), F32),
            vmem((2, n, 4, 8, span), F32),
            vmem((2, n, 4, 8, span), BF16),
            vmem((2, n, 4, 8, span), BF16),
            vmem((2, n, 2, 8, span), BF16),
            vmem((2, n, 2, 8, span), BF16),
            vmem((2, n, 8, span), BF16),
            vmem((2, n, 8, span), BF16),
            vmem((2, n, 4, 2, span), BF16),
            vmem((n, 4, 2, span), BF16),
            vmem((n, 4, 2, span), BF16),
            vmem((8, span), F32),
            vmem((n, 2, 4, 8, span), BF16),
            dma((5, max(n, 4))),
            dma(()),
            dma(()),
            dma((2, n)),
            dma((2, n)),
            dma((2, n)),
            dma((2, n)),
            dma((2, n)),
            dma((2, n)),
            dma((2, n, 4)),
            dma((n, 4)),
            dma((n, 3)),
            dma((n, 4)),
            dma((n, 3)),
            dma((n, 3)),
            dma((n, 4)),
            dma((n, 4)),
        ],
        compiler_params=pltpu.CompilerParams(
            collective_id=0, has_side_effects=True, vmem_limit_bytes=56 * 1024 * 1024
        ),
    )(ln_input[0], ln_grad[0], top_grad[0], ln_gain, hidden[0].T, master[0], moment[0], second[0])
    outs = pl.pallas_call(
        store,
        out_shape=tuple(jax.ShapeDtypeStruct(*r) for r in results),
        in_specs=[pl.BlockSpec(memory_space=vmem)] * 4,
        out_specs=(any_space,) * 4,
        scratch_shapes=[dma((4,))],
    )(*(pltpu.with_memory_space_constraint(out, vmem) for out in outs))
    return tuple(out[None] for out in outs)


def solution(mesh):
    n_section = mesh.shape["section"]
    finer = Mesh(mesh.devices.reshape(n_section, 4, 4, 2), ("section", *DP))
    rows = P("section", DP, None)
    return jax.shard_map(
        functools.partial(shards, n_section),
        mesh=finer,
        in_specs=(rows, rows, rows, P("section", None), rows, rows, rows, rows),
        out_specs=(rows, rows, rows, P("section", None, None)),
        check_vma=False,
    )
```
